32 devices in a mesh: rep: 1 (over z), mp: 4 (over y), tok: 8 (over x, core).
Axes of the slice: x: 4, y: 4, z: 1, core: 2. Of those that a mesh axis runs over, the one named last changes fastest.
The devices are a block of a 4x4x8 slice.
Arguments:
- x_in: bfloat16 [2, 8192, 2048], P(None, ('rep', 'tok', 'mp'))
- seg_ids: int32 [2, 8192], P(None, ('rep', 'tok', 'mp'))
- g_attn: bfloat16 [2, 2048], replicated
- w_q: bfloat16 [2, 2048, 32, 64], P(None, 'tok', 'mp')
- w_k: bfloat16 [2, 2048, 8, 64], P(None, 'tok', 'mp')
- w_v: bfloat16 [2, 2048, 8, 64], P(None, 'tok', 'mp')
- w_o: bfloat16 [2, 32, 64, 2048], P(None, 'mp', None, 'tok')
- g_mlp: bfloat16 [2, 2048], replicated
- w_gate: bfloat16 [2, 2048, 8192], P(None, 'tok', 'mp')
- w_up: bfloat16 [2, 2048, 8192], P(None, 'tok', 'mp')
- w_down: bfloat16 [2, 8192, 2048], P(None, 'mp', 'tok')
Outputs:
- output: float32 [2, 8192, 2048], P(None, ('rep', 'tok', 'mp'))
All inputs are finite; a program needn't handle non-finite values.
Results may differ from the reference program's by a relative error of at most 0.00825783.
Values are sent between devices in bfloat16 or wider.
A program may use at most 768 MiB of HBM per device.

```python
import jax
import jax.numpy as jnp
from jax import lax

EMBED_DIM = 2048
FFN_DIM = 8192
Q_HEADS = 32
KV_HEADS = 8
HEAD_DIM = 64
LAYERS = 2
MICRO_BATCHES = 2
NUM_SHARDS = 8
BLOCK_LEN = 1024
CUT_COUNT = 2
WAVE_COUNT = 4
TOKENS = NUM_SHARDS * BLOCK_LEN
BLOCKS = MICRO_BATCHES * NUM_SHARDS
NORM_EPS = 1e-5
ROPE_BASE = 10000.0
NEG_BIG = -1e30


def draw_segments(seg_key):
    cut_at = jax.random.randint(seg_key, (BLOCKS, CUT_COUNT), 1, BLOCK_LEN, dtype=jnp.int32)
    tok_order = jnp.arange(BLOCK_LEN, dtype=jnp.int32)
    is_start = jnp.any(tok_order[None, None, :] == cut_at[:, :, None], axis=1) | (tok_order[None, :] == 0)
    local_ids = jnp.cumsum(is_start.astype(jnp.int32), axis=1) - 1
    base_ids = jnp.arange(BLOCKS, dtype=jnp.int32)[:, None] * BLOCK_LEN
    return (local_ids + base_ids).astype(jnp.int32).reshape(MICRO_BATCHES, TOKENS)


def setup_inputs(seed: int = 0, part: int = 0) -> dict:
    root_key = jax.random.key(seed)
    key_list = jax.random.split(root_key, 12)
    part_key = jax.random.fold_in(key_list[0], part)
    noise_key, cos_key, sin_key, seg_key = jax.random.split(part_key, 4)
    freq_n = jnp.arange(1, WAVE_COUNT + 1, dtype=jnp.float32)
    t_frac = jnp.arange(BLOCK_LEN, dtype=jnp.float32) / BLOCK_LEN
    angles = 2.0 * jnp.pi * freq_n[:, None] * t_frac[None, :]
    amp_cos = jax.random.normal(cos_key, (BLOCKS, WAVE_COUNT, EMBED_DIM), jnp.float32)
    amp_sin = jax.random.normal(sin_key, (BLOCKS, WAVE_COUNT, EMBED_DIM), jnp.float32)
    smooth = (jnp.einsum('ks,bke->bse', jnp.cos(angles), amp_cos) + jnp.einsum('ks,bke->bse', jnp.sin(angles), amp_sin)) * WAVE_COUNT ** -0.5
    noise = jax.random.normal(noise_key, (BLOCKS, BLOCK_LEN, EMBED_DIM), jnp.float32)
    x_in = (0.8 * smooth + 0.6 * noise).reshape(MICRO_BATCHES, TOKENS, EMBED_DIM).astype(jnp.bfloat16)

    def weight(wkey, shape, fan_in):
        return (jax.random.normal(wkey, shape, jnp.float32) * fan_in ** -0.5).astype(jnp.bfloat16)

    def gains(wkey):
        return jax.random.uniform(wkey, (LAYERS, EMBED_DIM), jnp.float32, minval=0.5, maxval=1.5).astype(jnp.bfloat16)

    return {
        'x_in': x_in,
        'seg_ids': draw_segments(seg_key),
        'g_attn': gains(key_list[1]),
        'w_q': weight(key_list[2], (LAYERS, EMBED_DIM, Q_HEADS, HEAD_DIM), EMBED_DIM),
        'w_k': weight(key_list[3], (LAYERS, EMBED_DIM, KV_HEADS, HEAD_DIM), EMBED_DIM),
        'w_v': weight(key_list[4], (LAYERS, EMBED_DIM, KV_HEADS, HEAD_DIM), EMBED_DIM),
        'w_o': weight(key_list[5], (LAYERS, Q_HEADS, HEAD_DIM, EMBED_DIM), Q_HEADS * HEAD_DIM),
        'g_mlp': gains(key_list[6]),
        'w_gate': weight(key_list[7], (LAYERS, EMBED_DIM, FFN_DIM), EMBED_DIM),
        'w_up': weight(key_list[8], (LAYERS, EMBED_DIM, FFN_DIM), EMBED_DIM),
        'w_down': weight(key_list[9], (LAYERS, FFN_DIM, EMBED_DIM), FFN_DIM),
    }


def rms_norm(resid, gain_vec):
    mean_sq = jnp.mean(resid * resid, axis=-1, keepdims=True)
    return (resid * lax.rsqrt(mean_sq + NORM_EPS) * gain_vec.astype(jnp.float32)).astype(jnp.bfloat16)


def seg_positions(seg_rows):
    positions = jnp.arange(seg_rows.shape[-1], dtype=jnp.int32)
    previous = jnp.concatenate([seg_rows[..., :1] - 1, seg_rows[..., :-1]], axis=-1)
    start_at = jnp.where(seg_rows != previous, positions, 0)
    return positions - lax.cummax(start_at, axis=seg_rows.ndim - 1)


def rope_tables(positions, head_dim):
    half_dim = head_dim // 2
    inv_freq = ROPE_BASE ** (-2.0 * jnp.arange(half_dim, dtype=jnp.float32) / head_dim)
    angles = positions.astype(jnp.float32)[..., None] * inv_freq
    return jnp.cos(angles), jnp.sin(angles)


def apply_rope(values, cos_t, sin_t):
    half_dim = values.shape[-1] // 2
    first_half = values[..., :half_dim]
    second_half = values[..., half_dim:]
    return jnp.concatenate([first_half * cos_t - second_half * sin_t, second_half * cos_t + first_half * sin_t], axis=-1)


def block_attention(operands):
    q_blk, k_blk, v_blk, seg_blk = operands
    tok_order = jnp.arange(BLOCK_LEN)
    allowed = (seg_blk[:, None] == seg_blk[None, :]) & (tok_order[None, :] <= tok_order[:, None])

    def one_group(group_ops):
        q_grp, k_grp, v_grp = group_ops
        scores = jnp.einsum('sgd,td->sgt', q_grp.astype(jnp.float32), k_grp.astype(jnp.float32)) * HEAD_DIM ** -0.5
        scores = jnp.where(allowed[:, None, :], scores, NEG_BIG)
        probs_bf = jax.nn.softmax(scores, axis=-1).astype(jnp.bfloat16)
        return jnp.einsum('sgt,td->sgd', probs_bf.astype(jnp.float32), v_grp.astype(jnp.float32)).astype(jnp.bfloat16)

    group_out = lax.map(one_group, (jnp.moveaxis(q_blk, 1, 0), jnp.moveaxis(k_blk, 1, 0), jnp.moveaxis(v_blk, 1, 0)))
    return jnp.moveaxis(group_out, 0, 1)


def reference(x_in, seg_ids, g_attn, w_q, w_k, w_v, w_o, g_mlp, w_gate, w_up, w_down):
    groups = Q_HEADS // KV_HEADS
    seg_blocks = seg_ids.reshape(BLOCKS, BLOCK_LEN)
    cos_t, sin_t = rope_tables(seg_positions(seg_blocks), HEAD_DIM)
    cos_t = cos_t[:, :, None, :]
    sin_t = sin_t[:, :, None, :]

    def layer_step(residual, layer_w):
        ga_vec, wq_l, wk_l, wv_l, wo_l, gm_vec, wg_l, wu_l, wd_l = layer_w
        hidden = rms_norm(residual, ga_vec).reshape(BLOCKS, BLOCK_LEN, EMBED_DIM).astype(jnp.float32)
        q_lin = jnp.einsum('bse,end->bsnd', hidden, wq_l.astype(jnp.float32))
        k_lin = jnp.einsum('bse,end->bsnd', hidden, wk_l.astype(jnp.float32))
        v_lin = jnp.einsum('bse,end->bsnd', hidden, wv_l.astype(jnp.float32))
        q_rot = apply_rope(q_lin, cos_t, sin_t).astype(jnp.bfloat16).reshape(BLOCKS, BLOCK_LEN, KV_HEADS, groups, HEAD_DIM)
        k_rot = apply_rope(k_lin, cos_t, sin_t).astype(jnp.bfloat16)
        v_val = v_lin.astype(jnp.bfloat16)
        attn_out = lax.map(block_attention, (q_rot, k_rot, v_val, seg_blocks))
        attn_out = attn_out.reshape(BLOCKS, BLOCK_LEN, Q_HEADS, HEAD_DIM).astype(jnp.float32)
        proj_out = jnp.einsum('bsnd,nde->bse', attn_out, wo_l.astype(jnp.float32))
        residual = residual + proj_out.reshape(MICRO_BATCHES, TOKENS, EMBED_DIM)
        hidden = rms_norm(residual, gm_vec).reshape(MICRO_BATCHES * TOKENS, EMBED_DIM)
        gate_val = jnp.dot(hidden, wg_l, preferred_element_type=jnp.float32)
        up_val = jnp.dot(hidden, wu_l, preferred_element_type=jnp.float32)
        act_val = (jax.nn.silu(gate_val) * up_val).astype(jnp.bfloat16)
        down_val = jnp.dot(act_val, wd_l, preferred_element_type=jnp.float32)
        return residual + down_val.reshape(MICRO_BATCHES, TOKENS, EMBED_DIM), None

    final_res, _ = lax.scan(layer_step, x_in.astype(jnp.float32), (g_attn, w_q, w_k, w_v, w_o, g_mlp, w_gate, w_up, w_down))
    return final_res
```

```python
import functools

import jax
import jax.numpy as jnp
from jax import lax
from jax.experimental import pallas as pl
from jax.experimental.pallas import tpu as pltpu
from jax.sharding import PartitionSpec as P


NORM_EPS = 1e-5
ROPE_BASE = 10000.0
LOG2_E = 1.4426950408889634


def rope_tables(positions, head_dim):
    half_dim = head_dim // 2
    inv_freq = ROPE_BASE ** (-2.0 * jnp.arange(half_dim, dtype=jnp.float32) / head_dim)
    angles = positions.astype(jnp.float32)[..., None] * inv_freq
    cos_t, sin_t = jnp.cos(angles), jnp.sin(angles)
    cos_w = jnp.concatenate([cos_t] * 4, axis=-1)
    sin_w = jnp.concatenate([-sin_t, sin_t] * 2, axis=-1)
    return cos_w, sin_w


def norm_rows(resid, gain):
    mean_sq = jnp.mean(resid * resid, axis=-1, keepdims=True)
    return (resid * lax.rsqrt(mean_sq + NORM_EPS) * gain.astype(jnp.float32)).astype(jnp.bfloat16)


def rotate_pair(x, cos_w, sin_w, low):
    width = x.shape[-1]
    quarter = width // 4
    up = pltpu.roll(x, quarter, 1)
    down = pltpu.roll(x, width - quarter, 1)
    return (x * cos_w + jnp.where(low, down, up) * sin_w).astype(jnp.bfloat16)


def qkv_kernel(q_w, kv_w, resid_ref, gain_ref, cos_ref, sin_ref, w_ref, q_ref, kv_ref, hid):
    @pl.when(pl.program_id(0) == 0)
    def _():
        hid[...] = norm_rows(resid_ref[...].astype(jnp.float32), gain_ref[...])

    acc = jnp.dot(hid[...], w_ref[0], preferred_element_type=jnp.float32)
    cos_w, sin_w = cos_ref[...], sin_ref[...]
    pair = cos_w.shape[-1]
    lane = lax.broadcasted_iota(jnp.int32, cos_w.shape, 1)
    low = lax.rem(lane, pair // 2) < pair // 4
    for p in range(q_w // pair):
        q_ref[0, :, p * pair:(p + 1) * pair] = rotate_pair(acc[:, p * pair:(p + 1) * pair], cos_w, sin_w, low)
    for p in range(kv_w // pair):
        kv_ref[0, :, p * pair:(p + 1) * pair] = rotate_pair(
            acc[:, q_w + p * pair:q_w + (p + 1) * pair], cos_w, sin_w, low)
    kv_ref[0, :, kv_w:] = acc[:, q_w + kv_w:].astype(jnp.bfloat16)


def qkv_call(resid, gain, cos_w, sin_w, w_all):
    rows, embed = resid.shape
    shares, _, cols = w_all.shape
    kv_w = 128
    q_w = cols - 2 * kv_w
    pair = cos_w.shape[-1]
    return pl.pallas_call(
        functools.partial(qkv_kernel, q_w, kv_w),
        name="qkv",
        grid=(shares,),
        in_specs=[
            pl.BlockSpec((rows, embed), lambda m: (0, 0)),
            pl.BlockSpec((1, embed), lambda m: (0, 0)),
            pl.BlockSpec((rows, pair), lambda m: (0, 0)),
            pl.BlockSpec((rows, pair), lambda m: (0, 0)),
            pl.BlockSpec((1, embed, cols), lambda m: (m, 0, 0)),
        ],
        out_specs=[
            pl.BlockSpec((1, rows, q_w), lambda m: (m, 0, 0)),
            pl.BlockSpec((1, rows, 2 * kv_w), lambda m: (m, 0, 0)),
        ],
        out_shape=[
            jax.ShapeDtypeStruct((shares, rows, q_w), jnp.bfloat16),
            jax.ShapeDtypeStruct((shares, rows, 2 * kv_w), jnp.bfloat16),
        ],
        scratch_shapes=[pltpu.VMEM((rows, embed), jnp.bfloat16)],
        compiler_params=pltpu.CompilerParams(dimension_semantics=("arbitrary",), vmem_limit_bytes=40 * 1024 * 1024),
        cost_estimate=pl.CostEstimate(
            flops=2 * rows * embed * cols * shares, bytes_accessed=2 * embed * cols * shares, transcendentals=0),
    )(resid, gain, cos_w, sin_w, w_all)


def attn_kernel(score_c, q_ref, own_ref, left_ref, right_ref, opp_lo_ref, opp_hi_ref, bound_ref, wo_ref, resid_ref, gain_ref,
                out_ref, hid_ref, k_scr, v_scr, o_scr):
    step = pl.program_id(0)
    rows = q_ref.shape[1]
    pair = k_scr.shape[-1]
    half = pair // 2
    n_pairs = q_ref.shape[2] // pair
    lane = lax.broadcasted_iota(jnp.int32, (rows, pair), 1)
    low = lane < half
    zero = jnp.zeros((rows, pair), jnp.float32)

    def spread(c, kv_ref):
        at = slice(c * rows, (c + 1) * rows)
        for scr, lo in ((k_scr, 0), (v_scr, pair)):
            both = kv_ref[0, :, lo:lo + pair].astype(jnp.float32)
            swap = pltpu.roll(both, half, 1)
            scr[0, 0, at] = jnp.where(low, both, zero).astype(jnp.bfloat16)
            scr[0, 1, at] = jnp.where(low, zero, swap).astype(jnp.bfloat16)
            scr[1, 0, at] = jnp.where(low, swap, zero).astype(jnp.bfloat16)
            scr[1, 1, at] = jnp.where(low, zero, both).astype(jnp.bfloat16)

    spread(0, own_ref)
    spread(1, left_ref)
    spread(2, right_ref)
    first_half = step < pl.num_programs(0) // 2

    @pl.when(first_half)
    def _():
        spread(3, opp_lo_ref)

    @pl.when(jnp.logical_not(first_half))
    def _():
        spread(3, opp_hi_ref)

    def one_pair(p, carry):
        cols = pl.ds(pl.multiple_of(p * pair, pair), pair)
        q_pair = q_ref[0, :, cols]
        group = p // (n_pairs // 2)
        out = None
        for side in range(2):
            s = lax.dot_general(q_pair, k_scr[group, side], (((1,), (1,)), ((), ())),
                                preferred_element_type=jnp.float32)
            s = jnp.minimum(s, bound_ref[...]) * score_c
            e = jnp.exp2(s - jnp.max(s, axis=-1, keepdims=True))
            probs = (e * (1.0 / jnp.sum(e, axis=-1, keepdims=True))).astype(jnp.bfloat16)
            part = jnp.dot(probs, v_scr[group, side], preferred_element_type=jnp.float32)
            out = part if out is None else out + part
        o_scr[:, cols] = out.astype(jnp.bfloat16)
        return carry

    lax.fori_loop(0, n_pairs, one_pair, 0, unroll=2)

    @pl.when(step == 0)
    def _():
        out_ref[...] = resid_ref[...].astype(jnp.float32)

    tok_n, width = wo_ref.shape[1], wo_ref.shape[3]
    for t in range(tok_n):
        at = slice(t * width, (t + 1) * width)
        out_ref[:, at] += jnp.dot(o_scr[...], wo_ref[0, t], preferred_element_type=jnp.float32)

    @pl.when(step == pl.num_programs(0) - 1)
    def _():
        hid_ref[...] = norm_rows(out_ref[...], gain_ref[...])


def attn_call(q, kvs, bound, wo_all, resid, gain, head_dim):
    shares, rows, q_w = q.shape
    kv2 = kvs[0].shape[2]
    embed = resid.shape[1]
    pair = kv2 // 2
    keys = bound.shape[1]
    heads = shares * q_w // head_dim
    part = shares // 2
    whole = pl.BlockSpec((1, rows, kv2), lambda m: (m, 0, 0))
    return pl.pallas_call(
        functools.partial(attn_kernel, LOG2_E * head_dim ** -0.5),
        name="attn",
        grid=(shares,),
        in_specs=[
            pl.BlockSpec((1, rows, q_w), lambda m: (m, 0, 0)),
            whole, whole, whole,
            pl.BlockSpec((1, rows, kv2), lambda m: (jnp.minimum(m, part - 1), 0, 0)),
            pl.BlockSpec((1, rows, kv2), lambda m: (jnp.maximum(m - part, 0), 0, 0)),
            pl.BlockSpec((rows, keys), lambda m: (0, 0)),
            pl.BlockSpec((1,) + wo_all.shape[1:], lambda m: (m, 0, 0, 0)),
            pl.BlockSpec((rows, embed), lambda m: (0, 0)),
            pl.BlockSpec((1, embed), lambda m: (0, 0)),
        ],
        out_specs=[
            pl.BlockSpec((rows, embed), lambda m: (0, 0)),
            pl.BlockSpec((rows, embed), lambda m: (0, 0)),
        ],
        out_shape=[
            jax.ShapeDtypeStruct((rows, embed), jnp.float32),
            jax.ShapeDtypeStruct((rows, embed), jnp.bfloat16),
        ],
        scratch_shapes=[
            pltpu.VMEM((2, 2, keys, pair), jnp.bfloat16),
            pltpu.VMEM((2, 2, keys, pair), jnp.bfloat16),
            pltpu.VMEM((rows, q_w), jnp.bfloat16),
        ],
        compiler_params=pltpu.CompilerParams(dimension_semantics=("arbitrary",), vmem_limit_bytes=40 * 1024 * 1024),
        cost_estimate=pl.CostEstimate(
            flops=2 * rows * q_w * embed * shares + 16 * heads * rows * keys * head_dim,
            bytes_accessed=2 * q_w * embed * shares, transcendentals=heads * rows * keys),
    )(q, *kvs, bound, wo_all, resid, gain)


def mlp_kernel(n_in, n_out, n_act, *refs):
    ins = refs[:n_in]
    wg_ref, wu_ref, wd_ref = refs[n_in:n_in + 3]
    outs = refs[n_in + 3:n_in + 3 + n_out]
    x_scr, act_scr = refs[-2:]
    step = pl.program_id(0)

    @pl.when(step == 0)
    def _():
        at = 0
        for ref in ins:
            x_scr[at:at + ref.shape[0]] = ref[...]
            at += ref.shape[0]

    @pl.when(step < n_act)
    def _():
        gate = jnp.dot(x_scr[...], wg_ref[...], preferred_element_type=jnp.float32)
        up = jnp.dot(x_scr[...], wu_ref[...], preferred_element_type=jnp.float32)
        act_scr[step] = (jax.nn.silu(gate) * up).astype(jnp.bfloat16)

    @pl.when(step >= n_act)
    def _():
        rows = outs[0].shape[0]
        blk = act_scr.shape[2]
        part = None
        for i in range(n_act):
            term = jnp.dot(act_scr[i], wd_ref[i * blk:(i + 1) * blk], preferred_element_type=jnp.float32)
            part = term if part is None else part + term
        for i, ref in enumerate(outs):
            ref[...] = part[i * rows:(i + 1) * rows]


def mlp_call(pieces, n_out, w_g, w_u, w_d, blk=512, blk2=512):
    embed, ffn = w_g.shape
    total = sum(p.shape[0] for p in pieces)
    rows = total // n_out
    n_act = ffn // blk
    return pl.pallas_call(
        functools.partial(mlp_kernel, len(pieces), n_out, n_act),
        name="mlp",
        grid=(n_act + embed // blk2,),
        in_specs=[pl.BlockSpec(p.shape, lambda f: (0, 0)) for p in pieces]
        + [
            pl.BlockSpec((embed, blk), lambda f: (0, jnp.minimum(f, n_act - 1))),
            pl.BlockSpec((embed, blk), lambda f: (0, jnp.minimum(f, n_act - 1))),
            pl.BlockSpec((ffn, blk2), lambda f: (0, jnp.maximum(f - n_act, 0))),
        ],
        out_specs=[pl.BlockSpec((rows, blk2), lambda f: (0, jnp.maximum(f - n_act, 0)))] * n_out,
        out_shape=[jax.ShapeDtypeStruct((rows, embed), jnp.float32)] * n_out,
        scratch_shapes=[pltpu.VMEM((total, embed), jnp.bfloat16), pltpu.VMEM((n_act, total, blk), jnp.bfloat16)],
        compiler_params=pltpu.CompilerParams(dimension_semantics=("arbitrary",), vmem_limit_bytes=48 * 1024 * 1024),
        cost_estimate=pl.CostEstimate(
            flops=6 * total * embed * ffn, bytes_accessed=6 * embed * ffn, transcendentals=total * ffn),
    )(*pieces, w_g, w_u, w_d)


def gather_kernel(mp_n, x_n, n_pieces, *refs):
    pieces, outs = refs[:n_pieces], refs[n_pieces:2 * n_pieces]
    local_sems, send_sems, x_full, x_half, y_full, y_half, side_sems = refs[2 * n_pieces:]
    j, t = lax.axis_index('mp'), lax.axis_index('tok')
    x, core = t // 2, t % 2
    x_near = {1: {'tok': lax.rem(x + 1, x_n) * 2 + core}, -1: {'tok': lax.rem(x + x_n - 1, x_n) * 2 + core}}
    y_near = {1: {'mp': lax.rem(j + 1, mp_n)}, -1: {'mp': lax.rem(j + mp_n - 1, mp_n)}}
    other = {'tok': x * 2 + 1 - core}

    barrier = pltpu.get_barrier_semaphore()
    partners = [x_near[1], x_near[-1], y_near[1], y_near[-1], other]
    for who in partners:
        pl.semaphore_signal(barrier, inc=1, device_id=who, device_id_type=pl.DeviceIdType.MESH)
    pl.semaphore_wait(barrier, len(partners))

    order = (0, -1, 1, 2)
    place = {d: i for i, d in enumerate(order)}
    near = tuple(enumerate((-1, 1)))
    sent = []

    def unit(n, dx, dj, c=None):
        at_t = lax.rem(x + dx + x_n, x_n) * 2 + (core if c is None else c)
        return outs[n].at[lax.rem(j + dj + mp_n, mp_n), at_t]

    def part(n, i, ref):
        half = pieces[n].shape[0] // 2
        return ref.at[i * half:(i + 1) * half]

    def send(src, dst, sem, who):
        copy = pltpu.make_async_remote_copy(
            src_ref=src, dst_ref=dst, send_sem=send_sems.at[len(sent)], recv_sem=sem,
            device_id=who, device_id_type=pl.DeviceIdType.MESH)
        copy.start()
        sent.append(copy)

    def arrived(dst, sem, who):
        pltpu.make_async_remote_copy(
            src_ref=dst, dst_ref=dst, send_sem=send_sems.at[0], recv_sem=sem,
            device_id=who, device_id_type=pl.DeviceIdType.MESH).wait_recv()

    def side_sem(n, dx, dj):
        return side_sems.at[n * 16 + place[dx] * 4 + place[dj]]

    def to_side(n, dx, dj, src):
        send(src, unit(n, dx, dj), side_sem(n, dx, dj), other)

    def to_rows(n, dx, src):
        send(src, unit(n, dx, 0), y_full.at[n * 8 + place[dx] * 2], y_near[1])
        send(src, unit(n, dx, 0), y_full.at[n * 8 + place[dx] * 2 + 1], y_near[-1])

    every = range(n_pieces)
    kept = []
    for n in every:
        own = pieces[n]
        keep = pltpu.make_async_copy(own, unit(n, 0, 0), local_sems.at[n])
        keep.start()
        kept.append(keep)
        for i, d in near:
            send(own, unit(n, 0, 0), x_full.at[n * 2 + i], x_near[-d])
        to_rows(n, 0, own)
        to_side(n, 0, 0, own)
    for n in every:
        for i, d in near:
            got = unit(n, d, 0)
            arrived(got, x_full.at[n * 2 + i], x_near[d])
            send(part(n, i, got), part(n, i, got), x_half.at[n * 2 + i], x_near[-d])
            to_rows(n, d, got)
            to_side(n, d, 0, got)
    for n in every:
        got = unit(n, 2, 0)
        for i, d in near:
            arrived(part(n, i, got), x_half.at[n * 2 + i], x_near[d])
        to_rows(n, 2, got)
        to_side(n, 2, 0, got)
    for n in every:
        for dx in order:
            for i, d in near:
                got = unit(n, dx, d)
                at = n * 8 + place[dx] * 2 + i
                arrived(got, y_full.at[at], y_near[d])
                send(part(n, i, got), part(n, i, got), y_half.at[at], y_near[-d])
                to_side(n, dx, d, got)
    for n in every:
        for dx in order:
            got = unit(n, dx, 2)
            for i, d in near:
                arrived(part(n, i, got), y_half.at[n * 8 + place[dx] * 2 + i], y_near[d])
            to_side(n, dx, 2, got)
    for n in every:
        for dx in order:
            for dj in order:
                arrived(unit(n, dx, dj, 1 - core), side_sem(n, dx, dj), other)
    for copy in sent:
        copy.wait_send()
    for keep in kept:
        keep.wait()


def gather_call(pieces, mp_n, tok_n):
    n = len(pieces)
    n_sends = 5 + 2 * 4 + 3 + 8 * 2 + 4
    dma = pltpu.SemaphoreType.DMA
    return pl.pallas_call(
        functools.partial(gather_kernel, mp_n, tok_n // 2, n),
        name="gather_weights",
        in_specs=[pl.BlockSpec(memory_space=pltpu.VMEM)] * n,
        out_specs=[pl.BlockSpec(memory_space=pl.ANY)] * n,
        out_shape=[jax.ShapeDtypeStruct((mp_n, tok_n) + p.shape, p.dtype) for p in pieces],
        scratch_shapes=[dma((n,)), dma((n * n_sends,)), dma((2 * n,)), dma((2 * n,)), dma((8 * n,)), dma((8 * n,)), dma((16 * n,))],
        compiler_params=pltpu.CompilerParams(collective_id=1, has_side_effects=True),
        cost_estimate=pl.CostEstimate(
            flops=10 ** 11, bytes_accessed=sum(p.size for p in pieces) * 2 * mp_n * tok_n, transcendentals=0),
    )(*pieces)


def solution(mesh):
    act_spec = P(None, ('rep', 'tok', 'mp'), None)
    seg_spec = P(None, ('rep', 'tok', 'mp'))
    gain_spec = P(None, None)
    head_in = P(None, 'tok', 'mp', None)
    head_out = P(None, 'mp', None, 'tok')
    ffn_in = P(None, 'tok', 'mp')
    ffn_out = P(None, 'mp', 'tok')
    mp_n, tok_n = mesh.shape['mp'], mesh.shape['tok']
    fwd = [(i, (i + 1) % mp_n) for i in range(mp_n)]
    bwd = [(i, (i - 1) % mp_n) for i in range(mp_n)]

    def to_right(value):
        return lax.ppermute(value, 'mp', fwd)

    def to_left(value):
        return lax.ppermute(value, 'mp', bwd)

    def spread_ring(value):
        half = value.shape[0] // 2
        from_left, from_right = to_right(value), to_left(value)
        return [value, from_left, from_right,
                to_right(from_left[:half]), to_left(from_right[half:])]

    def device_fn(x_in, seg_ids, g_attn, w_q, w_k, w_v, w_o, g_mlp, w_gate, w_up, w_down):
        micro_n, rows, _ = x_in.shape
        layers = w_q.shape[0]
        head_dim = w_q.shape[3]
        e_part = w_q.shape[1]

        seg_parts = [seg_ids, to_right(seg_ids), to_left(seg_ids)]
        seg_parts.append(to_right(seg_parts[1]))
        weights = []
        for l in range(layers):
            w_qkv = jnp.concatenate([w[l].reshape(e_part, -1) for w in (w_q, w_k, w_v)], axis=1)
            w_o_l = w_o[l].reshape(-1, w_o.shape[3])
            if l == 0:
                w_qkv_all, w_o_all = gather_call([w_qkv, w_o_l], mp_n, tok_n)
            else:
                w_qkv_all = lax.all_gather(w_qkv, ('mp', 'tok'), axis=0)
                w_o_all = lax.all_gather(w_o_l, ('mp', 'tok'), axis=0).reshape((mp_n, tok_n) + w_o_l.shape)
            weights.append((
                w_qkv_all.reshape(mp_n, tok_n * e_part, -1), w_o_all,
                lax.all_gather(w_gate[l], 'tok', axis=0, tiled=True),
                lax.all_gather(w_up[l], 'tok', axis=0, tiled=True),
                lax.all_gather(w_down[l], 'tok', axis=1, tiled=True),
            ))

        me = lax.axis_index('mp')
        seg_ring = jnp.concatenate(seg_parts, axis=1)
        ring_at = [lax.rem(me + c + mp_n, mp_n) * rows for c in (0, -1, 1, 2)]
        key_at = jnp.concatenate([at + jnp.arange(rows, dtype=jnp.int32) for at in ring_at])
        own_at = key_at[:rows]
        streams = []
        for b in range(micro_n):
            same = seg_ring[b][None, :] == seg_ids[b][:, None]
            first = jnp.min(jnp.where(same, key_at[None, :], rows * mp_n), axis=1)
            cos_w, sin_w = rope_tables(own_at - first, head_dim)
            ok = same & (key_at[None, :] <= own_at[:, None])
            streams.append(dict(name='ab'[b], cos=cos_w, sin=sin_w, bound=jnp.where(ok, jnp.inf, -jnp.inf),
                                resid=x_in[b].astype(jnp.float32)))

        half = rows // 2
        last = [None]

        def in_turn(value, *more):
            held = [v for v in (last[0],) + more if v is not None]
            return lax.optimization_barrier((value, *held))[0] if held else value

        def qkv_step(st, l):
            resid = in_turn(st['resid'])
            q, kv = qkv_call(resid, g_attn[l:l + 1], st['cos'], st['sin'], weights[l][0])
            st['q'], st['kvs'] = q, spread_ring(kv)
            last[0] = kv

        def attn_step(st, l, *more):
            q = in_turn(st['q'], *more)
            st['resid'], hid = attn_call(q, st['kvs'], st['bound'], weights[l][1], st['resid'],
                                         g_mlp[l:l + 1], head_dim)
            st['hid'] = last[0] = hid

        def share_step(st, *more):
            hid = lax.optimization_barrier((st['hid'], *more))[0] if more else st['hid']
            st['hids'] = spread_ring(hid)

        def opp_step(st, l):
            lo, hi = st['hids'][3:]
            lo = in_turn(lo)
            (p_opp,) = mlp_call([lo, hi], 1, *weights[l][2:])
            st['opp_in'] = to_right(p_opp[:half]), to_left(p_opp[half:])
            last[0] = p_opp

        def near_step(st, l):
            own, left, right = st['hids'][:3]
            left = in_turn(left)
            p_own, p_left, p_right = mlp_call([own, left, right], 3, *weights[l][2:])
            last[0] = p_own
            lo_in, hi_in = st['opp_in']
            p_right = jnp.concatenate([p_right[:half] + lo_in, p_right[half:]], axis=0)
            p_left = jnp.concatenate([p_left[:half], p_left[half:] + hi_in], axis=0)
            st['relay'] = p_right
            st['resid'] = st['resid'] + p_own + to_right(p_right) + to_left(p_left)

        a, b = streams
        for l in range(layers):
            qkv_step(a, l)
            if l == 0:
                qkv_step(b, l)
                attn_step(a, l)
                share_step(a)
                attn_step(b, l)
                share_step(b, *a['hids'][1:3])
                opp_step(a, l)
                near_step(a, l)
            else:
                attn_step(a, l, b['relay'])
                share_step(a)
                qkv_step(b, l)
                opp_step(a, l)
                attn_step(b, l)
                share_step(b)
                near_step(a, l)
            opp_step(b, l)
            near_step(b, l)
        return jnp.stack([st['resid'] for st in streams])


    return jax.shard_map(
        device_fn,
        mesh=mesh,
        in_specs=(act_spec, seg_spec, gain_spec, head_in, head_in, head_in, head_out, gain_spec, ffn_in, ffn_in, ffn_out),
        out_specs=act_spec,
        check_vma=False,
    )
```

```python
import functools

import jax
import jax.numpy as jnp
from jax import lax
from jax.experimental import pallas as pl
from jax.experimental.pallas import tpu as pltpu
from jax.sharding import PartitionSpec as P


NORM_EPS = 1e-5
ROPE_BASE = 10000.0
LOG2_E = 1.4426950408889634


def rope_tables(positions, head_dim):
    half_dim = head_dim // 2
    inv_freq = ROPE_BASE ** (-2.0 * jnp.arange(half_dim, dtype=jnp.float32) / head_dim)
    angles = positions.astype(jnp.float32)[..., None] * inv_freq
    cos_t, sin_t = jnp.cos(angles), jnp.sin(angles)
    cos_w = jnp.concatenate([cos_t] * 4, axis=-1)
    sin_w = jnp.concatenate([-sin_t, sin_t] * 2, axis=-1)
    return cos_w, sin_w


def norm_rows(resid, gain):
    mean_sq = jnp.mean(resid * resid, axis=-1, keepdims=True)
    return (resid * lax.rsqrt(mean_sq + NORM_EPS) * gain.astype(jnp.float32)).astype(jnp.bfloat16)


def rotate_pair(x, cos_w, sin_w, low):
    width = x.shape[-1]
    quarter = width // 4
    up = pltpu.roll(x, quarter, 1)
    down = pltpu.roll(x, width - quarter, 1)
    return (x * cos_w + jnp.where(low, down, up) * sin_w).astype(jnp.bfloat16)


def qkv_kernel(q_w, kv_w, resid_ref, gain_ref, cos_ref, sin_ref, w_ref, q_ref, kv_ref, hid):
    @pl.when(pl.program_id(0) == 0)
    def _():
        hid[...] = norm_rows(resid_ref[...].astype(jnp.float32), gain_ref[...])

    acc = jnp.dot(hid[...], w_ref[0], preferred_element_type=jnp.float32)
    cos_w, sin_w = cos_ref[...], sin_ref[...]
    pair = cos_w.shape[-1]
    lane = lax.broadcasted_iota(jnp.int32, cos_w.shape, 1)
    low = lax.rem(lane, pair // 2) < pair // 4
    for p in range(q_w // pair):
        q_ref[0, :, p * pair:(p + 1) * pair] = rotate_pair(acc[:, p * pair:(p + 1) * pair], cos_w, sin_w, low)
    for p in range(kv_w // pair):
        kv_ref[0, :, p * pair:(p + 1) * pair] = rotate_pair(
            acc[:, q_w + p * pair:q_w + (p + 1) * pair], cos_w, sin_w, low)
    kv_ref[0, :, kv_w:] = acc[:, q_w + kv_w:].astype(jnp.bfloat16)


def qkv_call(resid, gain, cos_w, sin_w, w_all):
    rows, embed = resid.shape
    shares, _, cols = w_all.shape
    kv_w = 128
    q_w = cols - 2 * kv_w
    pair = cos_w.shape[-1]
    return pl.pallas_call(
        functools.partial(qkv_kernel, q_w, kv_w),
        name="qkv",
        grid=(shares,),
        in_specs=[
            pl.BlockSpec((rows, embed), lambda m: (0, 0)),
            pl.BlockSpec((1, embed), lambda m: (0, 0)),
            pl.BlockSpec((rows, pair), lambda m: (0, 0)),
            pl.BlockSpec((rows, pair), lambda m: (0, 0)),
            pl.BlockSpec((1, embed, cols), lambda m: (m, 0, 0)),
        ],
        out_specs=[
            pl.BlockSpec((1, rows, q_w), lambda m: (m, 0, 0)),
            pl.BlockSpec((1, rows, 2 * kv_w), lambda m: (m, 0, 0)),
        ],
        out_shape=[
            jax.ShapeDtypeStruct((shares, rows, q_w), jnp.bfloat16),
            jax.ShapeDtypeStruct((shares, rows, 2 * kv_w), jnp.bfloat16),
        ],
        scratch_shapes=[pltpu.VMEM((rows, embed), jnp.bfloat16)],
        compiler_params=pltpu.CompilerParams(dimension_semantics=("arbitrary",), vmem_limit_bytes=40 * 1024 * 1024),
        cost_estimate=pl.CostEstimate(
            flops=2 * rows * embed * cols * shares, bytes_accessed=2 * embed * cols * shares, transcendentals=0),
    )(resid, gain, cos_w, sin_w, w_all)


def attn_kernel(score_c, q_ref, own_ref, left_ref, right_ref, opp_lo_ref, opp_hi_ref, bound_ref, wo_ref, resid_ref, gain_ref,
                out_ref, hid_ref, k_scr, v_scr, o_scr):
    step = pl.program_id(0)
    rows = q_ref.shape[1]
    pair = k_scr.shape[-1]
    half = pair // 2
    n_pairs = q_ref.shape[2] // pair
    lane = lax.broadcasted_iota(jnp.int32, (rows, pair), 1)
    low = lane < half
    zero = jnp.zeros((rows, pair), jnp.float32)

    def spread(c, kv_ref):
        at = slice(c * rows, (c + 1) * rows)
        for scr, lo in ((k_scr, 0), (v_scr, pair)):
            both = kv_ref[0, :, lo:lo + pair].astype(jnp.float32)
            swap = pltpu.roll(both, half, 1)
            scr[0, 0, at] = jnp.where(low, both, zero).astype(jnp.bfloat16)
            scr[0, 1, at] = jnp.where(low, zero, swap).astype(jnp.bfloat16)
            scr[1, 0, at] = jnp.where(low, swap, zero).astype(jnp.bfloat16)
            scr[1, 1, at] = jnp.where(low, zero, both).astype(jnp.bfloat16)

    spread(0, own_ref)
    spread(1, left_ref)
    spread(2, right_ref)
    first_half = step < pl.num_programs(0) // 2

    @pl.when(first_half)
    def _():
        spread(3, opp_lo_ref)

    @pl.when(jnp.logical_not(first_half))
    def _():
        spread(3, opp_hi_ref)

    def one_pair(p, carry):
        cols = pl.ds(pl.multiple_of(p * pair, pair), pair)
        q_pair = q_ref[0, :, cols]
        group = p // (n_pairs // 2)
        out = None
        for side in range(2):
            s = lax.dot_general(q_pair, k_scr[group, side], (((1,), (1,)), ((), ())),
                                preferred_element_type=jnp.float32)
            s = jnp.minimum(s, bound_ref[...]) * score_c
            e = jnp.exp2(s - jnp.max(s, axis=-1, keepdims=True))
            probs = (e * (1.0 / jnp.sum(e, axis=-1, keepdims=True))).astype(jnp.bfloat16)
            part = jnp.dot(probs, v_scr[group, side], preferred_element_type=jnp.float32)
            out = part if out is None else out + part
        o_scr[:, cols] = out.astype(jnp.bfloat16)
        return carry

    lax.fori_loop(0, n_pairs, one_pair, 0, unroll=2)

    @pl.when(step == 0)
    def _():
        out_ref[...] = resid_ref[...].astype(jnp.float32)

    tok_n, width = wo_ref.shape[1], wo_ref.shape[3]
    for t in range(tok_n):
        at = slice(t * width, (t + 1) * width)
        out_ref[:, at] += jnp.dot(o_scr[...], wo_ref[0, t], preferred_element_type=jnp.float32)

    @pl.when(step == pl.num_programs(0) - 1)
    def _():
        hid_ref[...] = norm_rows(out_ref[...], gain_ref[...])


def attn_call(q, kvs, bound, wo_all, resid, gain, head_dim):
    shares, rows, q_w = q.shape
    kv2 = kvs[0].shape[2]
    embed = resid.shape[1]
    pair = kv2 // 2
    keys = bound.shape[1]
    heads = shares * q_w // head_dim
    part = shares // 2
    whole = pl.BlockSpec((1, rows, kv2), lambda m: (m, 0, 0))
    return pl.pallas_call(
        functools.partial(attn_kernel, LOG2_E * head_dim ** -0.5),
        name="attn",
        grid=(shares,),
        in_specs=[
            pl.BlockSpec((1, rows, q_w), lambda m: (m, 0, 0)),
            whole, whole, whole,
            pl.BlockSpec((1, rows, kv2), lambda m: (jnp.minimum(m, part - 1), 0, 0)),
            pl.BlockSpec((1, rows, kv2), lambda m: (jnp.maximum(m - part, 0), 0, 0)),
            pl.BlockSpec((rows, keys), lambda m: (0, 0)),
            pl.BlockSpec((1,) + wo_all.shape[1:], lambda m: (m, 0, 0, 0)),
            pl.BlockSpec((rows, embed), lambda m: (0, 0)),
            pl.BlockSpec((1, embed), lambda m: (0, 0)),
        ],
        out_specs=[
            pl.BlockSpec((rows, embed), lambda m: (0, 0)),
            pl.BlockSpec((rows, embed), lambda m: (0, 0)),
        ],
        out_shape=[
            jax.ShapeDtypeStruct((rows, embed), jnp.float32),
            jax.ShapeDtypeStruct((rows, embed), jnp.bfloat16),
        ],
        scratch_shapes=[
            pltpu.VMEM((2, 2, keys, pair), jnp.bfloat16),
            pltpu.VMEM((2, 2, keys, pair), jnp.bfloat16),
            pltpu.VMEM((rows, q_w), jnp.bfloat16),
        ],
        compiler_params=pltpu.CompilerParams(dimension_semantics=("arbitrary",), vmem_limit_bytes=40 * 1024 * 1024),
        cost_estimate=pl.CostEstimate(
            flops=2 * rows * q_w * embed * shares + 16 * heads * rows * keys * head_dim,
            bytes_accessed=2 * q_w * embed * shares, transcendentals=heads * rows * keys),
    )(q, *kvs, bound, wo_all, resid, gain)


def mlp_kernel(n_in, n_out, n_act, *refs):
    ins = refs[:n_in]
    wg_ref, wu_ref, wd_ref = refs[n_in:n_in + 3]
    outs = refs[n_in + 3:n_in + 3 + n_out]
    x_scr, act_scr = refs[-2:]
    step = pl.program_id(0)

    @pl.when(step == 0)
    def _():
        at = 0
        for ref in ins:
            x_scr[at:at + ref.shape[0]] = ref[...]
            at += ref.shape[0]

    @pl.when(step < n_act)
    def _():
        gate = jnp.dot(x_scr[...], wg_ref[...], preferred_element_type=jnp.float32)
        up = jnp.dot(x_scr[...], wu_ref[...], preferred_element_type=jnp.float32)
        act_scr[step] = (jax.nn.silu(gate) * up).astype(jnp.bfloat16)

    @pl.when(step >= n_act)
    def _():
        rows = outs[0].shape[0]
        blk = act_scr.shape[2]
        part = None
        for i in range(n_act):
            term = jnp.dot(act_scr[i], wd_ref[i * blk:(i + 1) * blk], preferred_element_type=jnp.float32)
            part = term if part is None else part + term
        for i, ref in enumerate(outs):
            ref[...] = part[i * rows:(i + 1) * rows]


def mlp_call(pieces, n_out, w_g, w_u, w_d, blk=512, blk2=512):
    embed, ffn = w_g.shape
    total = sum(p.shape[0] for p in pieces)
    rows = total // n_out
    n_act = ffn // blk
    return pl.pallas_call(
        functools.partial(mlp_kernel, len(pieces), n_out, n_act),
        name="mlp",
        grid=(n_act + embed // blk2,),
        in_specs=[pl.BlockSpec(p.shape, lambda f: (0, 0)) for p in pieces]
        + [
            pl.BlockSpec((embed, blk), lambda f: (0, jnp.minimum(f, n_act - 1))),
            pl.BlockSpec((embed, blk), lambda f: (0, jnp.minimum(f, n_act - 1))),
            pl.BlockSpec((ffn, blk2), lambda f: (0, jnp.maximum(f - n_act, 0))),
        ],
        out_specs=[pl.BlockSpec((rows, blk2), lambda f: (0, jnp.maximum(f - n_act, 0)))] * n_out,
        out_shape=[jax.ShapeDtypeStruct((rows, embed), jnp.float32)] * n_out,
        scratch_shapes=[pltpu.VMEM((total, embed), jnp.bfloat16), pltpu.VMEM((n_act, total, blk), jnp.bfloat16)],
        compiler_params=pltpu.CompilerParams(dimension_semantics=("arbitrary",), vmem_limit_bytes=48 * 1024 * 1024),
        cost_estimate=pl.CostEstimate(
            flops=6 * total * embed * ffn, bytes_accessed=6 * embed * ffn, transcendentals=total * ffn),
    )(*pieces, w_g, w_u, w_d)


def gather_kernel(mp_n, x_n, n_pieces, *refs):
    pieces, outs = refs[:n_pieces], refs[n_pieces:2 * n_pieces]
    local_sems, send_sems, x_full, x_half, y_full, y_half, side_sems = refs[2 * n_pieces:]
    j, t = lax.axis_index('mp'), lax.axis_index('tok')
    x, core = t // 2, t % 2
    x_near = {1: {'tok': lax.rem(x + 1, x_n) * 2 + core}, -1: {'tok': lax.rem(x + x_n - 1, x_n) * 2 + core}}
    y_near = {1: {'mp': lax.rem(j + 1, mp_n)}, -1: {'mp': lax.rem(j + mp_n - 1, mp_n)}}
    other = {'tok': x * 2 + 1 - core}

    barrier = pltpu.get_barrier_semaphore()
    partners = [x_near[1], x_near[-1], y_near[1], y_near[-1], other]
    for who in partners:
        pl.semaphore_signal(barrier, inc=1, device_id=who, device_id_type=pl.DeviceIdType.MESH)
    pl.semaphore_wait(barrier, len(partners))

    order = (0, -1, 1, 2)
    place = {d: i for i, d in enumerate(order)}
    near = tuple(enumerate((-1, 1)))
    sent = []

    def unit(n, dx, dj, c=None):
        at_t = lax.rem(x + dx + x_n, x_n) * 2 + (core if c is None else c)
        return outs[n].at[lax.rem(j + dj + mp_n, mp_n), at_t]

    def part(n, i, ref):
        half = pieces[n].shape[0] // 2
        return ref.at[i * half:(i + 1) * half]

    def send(src, dst, sem, who):
        copy = pltpu.make_async_remote_copy(
            src_ref=src, dst_ref=dst, send_sem=send_sems.at[len(sent)], recv_sem=sem,
            device_id=who, device_id_type=pl.DeviceIdType.MESH)
        copy.start()
        sent.append(copy)

    def arrived(dst, sem, who):
        pltpu.make_async_remote_copy(
            src_ref=dst, dst_ref=dst, send_sem=send_sems.at[0], recv_sem=sem,
            device_id=who, device_id_type=pl.DeviceIdType.MESH).wait_recv()

    def side_sem(n, dx, dj):
        return side_sems.at[n * 16 + place[dx] * 4 + place[dj]]

    def to_side(n, dx, dj, src):
        send(src, unit(n, dx, dj), side_sem(n, dx, dj), other)

    def to_rows(n, dx, src):
        send(src, unit(n, dx, 0), y_full.at[n * 8 + place[dx] * 2], y_near[1])
        send(src, unit(n, dx, 0), y_full.at[n * 8 + place[dx] * 2 + 1], y_near[-1])

    every = range(n_pieces)
    kept = []
    for n in every:
        own = pieces[n]
        keep = pltpu.make_async_copy(own, unit(n, 0, 0), local_sems.at[n])
        keep.start()
        kept.append(keep)
        for i, d in near:
            send(own, unit(n, 0, 0), x_full.at[n * 2 + i], x_near[-d])
        to_rows(n, 0, own)
        to_side(n, 0, 0, own)
    for n in every:
        for i, d in near:
            got = unit(n, d, 0)
            arrived(got, x_full.at[n * 2 + i], x_near[d])
            send(part(n, i, got), part(n, i, got), x_half.at[n * 2 + i], x_near[-d])
            to_rows(n, d, got)
            to_side(n, d, 0, got)
    for n in every:
        got = unit(n, 2, 0)
        for i, d in near:
            arrived(part(n, i, got), x_half.at[n * 2 + i], x_near[d])
        to_rows(n, 2, got)
        to_side(n, 2, 0, got)
    for n in every:
        for dx in order:
            for i, d in near:
                got = unit(n, dx, d)
                at = n * 8 + place[dx] * 2 + i
                arrived(got, y_full.at[at], y_near[d])
                send(part(n, i, got), part(n, i, got), y_half.at[at], y_near[-d])
                to_side(n, dx, d, got)
    for n in every:
        for dx in order:
            got = unit(n, dx, 2)
            for i, d in near:
                arrived(part(n, i, got), y_half.at[n * 8 + place[dx] * 2 + i], y_near[d])
            to_side(n, dx, 2, got)
    for n in every:
        for dx in order:
            for dj in order:
                arrived(unit(n, dx, dj, 1 - core), side_sem(n, dx, dj), other)
    for copy in sent:
        copy.wait_send()
    for keep in kept:
        keep.wait()


def gather_call(pieces, mp_n, tok_n):
    n = len(pieces)
    n_sends = 5 + 2 * 4 + 3 + 8 * 2 + 4
    dma = pltpu.SemaphoreType.DMA
    return pl.pallas_call(
        functools.partial(gather_kernel, mp_n, tok_n // 2, n),
        name="gather_weights",
        in_specs=[pl.BlockSpec(memory_space=pltpu.VMEM)] * n,
        out_specs=[pl.BlockSpec(memory_space=pl.ANY)] * n,
        out_shape=[jax.ShapeDtypeStruct((mp_n, tok_n) + p.shape, p.dtype) for p in pieces],
        scratch_shapes=[dma((n,)), dma((n * n_sends,)), dma((2 * n,)), dma((2 * n,)), dma((8 * n,)), dma((8 * n,)), dma((16 * n,))],
        compiler_params=pltpu.CompilerParams(collective_id=1, has_side_effects=True),
        cost_estimate=pl.CostEstimate(
            flops=10 ** 11, bytes_accessed=sum(p.size for p in pieces) * 2 * mp_n * tok_n, transcendentals=0),
    )(*pieces)


def solution(mesh):
    act_spec = P(None, ('rep', 'tok', 'mp'), None)
    seg_spec = P(None, ('rep', 'tok', 'mp'))
    gain_spec = P(None, None)
    head_in = P(None, 'tok', 'mp', None)
    head_out = P(None, 'mp', None, 'tok')
    ffn_in = P(None, 'tok', 'mp')
    ffn_out = P(None, 'mp', 'tok')
    mp_n, tok_n = mesh.shape['mp'], mesh.shape['tok']
    fwd = [(i, (i + 1) % mp_n) for i in range(mp_n)]
    bwd = [(i, (i - 1) % mp_n) for i in range(mp_n)]

    def to_right(value):
        return lax.ppermute(value, 'mp', fwd)

    def to_left(value):
        return lax.ppermute(value, 'mp', bwd)

    def spread_ring(value):
        half = value.shape[0] // 2
        from_left, from_right = to_right(value), to_left(value)
        return [value, from_left, from_right,
                to_right(from_left[:half]), to_left(from_right[half:])]

    def body(x_in, seg_ids, g_attn, w_q, w_k, w_v, w_o, g_mlp, w_gate, w_up, w_down):
        micro_n, rows, _ = x_in.shape
        layers = w_q.shape[0]
        head_dim = w_q.shape[3]
        e_part = w_q.shape[1]

        seg_parts = [seg_ids, to_right(seg_ids), to_left(seg_ids)]
        seg_parts.append(to_right(seg_parts[1]))
        me = lax.axis_index('mp')
        seg_ring = jnp.concatenate(seg_parts, axis=1)
        ring_at = [lax.rem(me + c + mp_n, mp_n) * rows for c in (0, -1, 1, 2)]
        key_at = jnp.concatenate([at + jnp.arange(rows, dtype=jnp.int32) for at in ring_at])
        own_at = key_at[:rows]
        streams = []
        for b in range(micro_n):
            same = seg_ring[b][None, :] == seg_ids[b][:, None]
            first = jnp.min(jnp.where(same, key_at[None, :], rows * mp_n), axis=1)
            cos_w, sin_w = rope_tables(own_at - first, head_dim)
            ok = same & (key_at[None, :] <= own_at[:, None])
            streams.append(dict(name='ab'[b], cos=cos_w, sin=sin_w, bound=jnp.where(ok, jnp.inf, -jnp.inf),
                                resid=x_in[b].astype(jnp.float32)))

        def gathered(value, axis_name, **how):
            return lax.all_gather(value, axis_name, **how)

        weights = []
        for l in range(layers):
            w_qkv = jnp.concatenate([w[l].reshape(e_part, -1) for w in (w_q, w_k, w_v)], axis=1)
            w_o_l = w_o[l].reshape(-1, w_o.shape[3])
            if l == 0:
                w_qkv, w_o_l, *_ = lax.optimization_barrier(
                    (w_qkv, w_o_l, *[st[k] for st in streams for k in ('cos', 'sin')]))
                w_qkv_all, w_o_all = gather_call([w_qkv, w_o_l], mp_n, tok_n)
                w_qkv_all = w_qkv_all.reshape(mp_n, tok_n * e_part, -1)
            else:
                w_qkv_all = gathered(gathered(w_qkv, 'mp', axis=0), 'tok', axis=1, tiled=True)
                w_o_all = gathered(gathered(w_o_l, 'mp', axis=0), 'tok', axis=1)
            weights.append((
                w_qkv_all, w_o_all,
                gathered(w_gate[l], 'tok', axis=0, tiled=True),
                gathered(w_up[l], 'tok', axis=0, tiled=True),
                gathered(w_down[l], 'tok', axis=1, tiled=True),
            ))

        half = rows // 2
        last = [None]

        def in_turn(value, *more):
            held = [v for v in (last[0],) + more if v is not None]
            return lax.optimization_barrier((value, *held))[0] if held else value

        def qkv_step(st, l):
            resid = in_turn(st['resid'])
            q, kv = qkv_call(resid, g_attn[l:l + 1], st['cos'], st['sin'], weights[l][0])
            st['q'], st['kvs'] = q, spread_ring(kv)
            last[0] = kv

        def attn_step(st, l, *more):
            q = in_turn(st['q'], *more)
            st['resid'], hid = attn_call(q, st['kvs'], st['bound'], weights[l][1], st['resid'],
                                         g_mlp[l:l + 1], head_dim)
            st['hid'] = last[0] = hid

        def share_step(st, *more):
            hid = lax.optimization_barrier((st['hid'], *more))[0] if more else st['hid']
            st['hids'] = spread_ring(hid)

        def opp_step(st, l):
            lo, hi = st['hids'][3:]
            lo = in_turn(lo)
            (p_opp,) = mlp_call([lo, hi], 1, *weights[l][2:])
            st['opp_in'] = to_right(p_opp[:half]), to_left(p_opp[half:])
            last[0] = p_opp

        def near_step(st, l):
            own, left, right = st['hids'][:3]
            left = in_turn(left)
            p_own, p_left, p_right = mlp_call([own, left, right], 3, *weights[l][2:])
            last[0] = p_own
            lo_in, hi_in = st['opp_in']
            p_right = jnp.concatenate([p_right[:half] + lo_in, p_right[half:]], axis=0)
            p_left = jnp.concatenate([p_left[:half], p_left[half:] + hi_in], axis=0)
            st['relay'] = p_right
            st['resid'] = st['resid'] + p_own + to_right(p_right) + to_left(p_left)

        a, b = streams
        for l in range(layers):
            qkv_step(a, l)
            if l == 0:
                qkv_step(b, l)
                attn_step(a, l)
                share_step(a)
                attn_step(b, l)
                share_step(b, *a['hids'][1:3])
                opp_step(a, l)
                near_step(a, l)
            else:
                attn_step(a, l)
                share_step(a)
                qkv_step(b, l)
                opp_step(a, l)
                attn_step(b, l)
                share_step(b)
                near_step(a, l)
            opp_step(b, l)
            near_step(b, l)
        return jnp.stack([st['resid'] for st in streams])


    return jax.shard_map(
        body,
        mesh=mesh,
        in_specs=(act_spec, seg_spec, gain_spec, head_in, head_in, head_in, head_out, gain_spec, ffn_in, ffn_in, ffn_out),
        out_specs=act_spec,
        check_vma=False,
    )
```

```python
import functools

import jax
import jax.numpy as jnp
from jax import lax
from jax.experimental import pallas as pl
from jax.experimental.pallas import tpu as pltpu
from jax.sharding import PartitionSpec as P


NORM_EPS = 1e-5
ROPE_BASE = 10000.0
LOG2_E = 1.4426950408889634


def rope_tables(positions, head_dim):
    half_dim = head_dim // 2
    inv_freq = ROPE_BASE ** (-2.0 * jnp.arange(half_dim, dtype=jnp.float32) / head_dim)
    angles = positions.astype(jnp.float32)[..., None] * inv_freq
    cos_t, sin_t = jnp.cos(angles), jnp.sin(angles)
    cos_w = jnp.concatenate([cos_t] * 4, axis=-1)
    sin_w = jnp.concatenate([-sin_t, sin_t] * 2, axis=-1)
    return cos_w, sin_w


def norm_rows(resid, gain):
    mean_sq = jnp.mean(resid * resid, axis=-1, keepdims=True)
    return (resid * lax.rsqrt(mean_sq + NORM_EPS) * gain.astype(jnp.float32)).astype(jnp.bfloat16)


def rotate_pair(x, cos_w, sin_w, low):
    width = x.shape[-1]
    quarter = width // 4
    up = pltpu.roll(x, quarter, 1)
    down = pltpu.roll(x, width - quarter, 1)
    return (x * cos_w + jnp.where(low, down, up) * sin_w).astype(jnp.bfloat16)


def qkv_kernel(q_w, kv_w, resid_ref, gain_ref, cos_ref, sin_ref, w_ref, q_ref, kv_ref, hid):
    @pl.when(pl.program_id(0) == 0)
    def _():
        hid[...] = norm_rows(resid_ref[...].astype(jnp.float32), gain_ref[...])

    acc = jnp.dot(hid[...], w_ref[0], preferred_element_type=jnp.float32)
    cos_w, sin_w = cos_ref[...], sin_ref[...]
    pair = cos_w.shape[-1]
    lane = lax.broadcasted_iota(jnp.int32, cos_w.shape, 1)
    low = lax.rem(lane, pair // 2) < pair // 4
    for p in range(q_w // pair):
        q_ref[0, :, p * pair:(p + 1) * pair] = rotate_pair(acc[:, p * pair:(p + 1) * pair], cos_w, sin_w, low)
    for p in range(kv_w // pair):
        kv_ref[0, :, p * pair:(p + 1) * pair] = rotate_pair(
            acc[:, q_w + p * pair:q_w + (p + 1) * pair], cos_w, sin_w, low)
    kv_ref[0, :, kv_w:] = acc[:, q_w + kv_w:].astype(jnp.bfloat16)


def qkv_call(resid, gain, cos_w, sin_w, w_all):
    rows, embed = resid.shape
    shares, _, cols = w_all.shape
    kv_w = 128
    q_w = cols - 2 * kv_w
    pair = cos_w.shape[-1]
    return pl.pallas_call(
        functools.partial(qkv_kernel, q_w, kv_w),
        name="qkv",
        grid=(shares,),
        in_specs=[
            pl.BlockSpec((rows, embed), lambda m: (0, 0)),
            pl.BlockSpec((1, embed), lambda m: (0, 0)),
            pl.BlockSpec((rows, pair), lambda m: (0, 0)),
            pl.BlockSpec((rows, pair), lambda m: (0, 0)),
            pl.BlockSpec((1, embed, cols), lambda m: (m, 0, 0)),
        ],
        out_specs=[
            pl.BlockSpec((1, rows, q_w), lambda m: (m, 0, 0)),
            pl.BlockSpec((1, rows, 2 * kv_w), lambda m: (m, 0, 0)),
        ],
        out_shape=[
            jax.ShapeDtypeStruct((shares, rows, q_w), jnp.bfloat16),
            jax.ShapeDtypeStruct((shares, rows, 2 * kv_w), jnp.bfloat16),
        ],
        scratch_shapes=[pltpu.VMEM((rows, embed), jnp.bfloat16)],
        compiler_params=pltpu.CompilerParams(dimension_semantics=("arbitrary",), vmem_limit_bytes=40 * 1024 * 1024),
        cost_estimate=pl.CostEstimate(
            flops=2 * rows * embed * cols * shares, bytes_accessed=2 * embed * cols * shares, transcendentals=0),
    )(resid, gain, cos_w, sin_w, w_all)


def attn_kernel(score_c, q_ref, own_ref, left_ref, right_ref, opp_lo_ref, opp_hi_ref, bound_ref, wo_ref, resid_ref, gain_ref,
                out_ref, hid_ref, k_scr, v_scr, o_scr):
    step = pl.program_id(0)
    rows = q_ref.shape[1]
    pair = k_scr.shape[-1]
    half = pair // 2
    n_pairs = q_ref.shape[2] // pair
    lane = lax.broadcasted_iota(jnp.int32, (rows, pair), 1)
    low = lane < half
    zero = jnp.zeros((rows, pair), jnp.float32)

    def spread(c, kv_ref):
        at = slice(c * rows, (c + 1) * rows)
        for scr, lo in ((k_scr, 0), (v_scr, pair)):
            both = kv_ref[0, :, lo:lo + pair].astype(jnp.float32)
            swap = pltpu.roll(both, half, 1)
            scr[0, 0, at] = jnp.where(low, both, zero).astype(jnp.bfloat16)
            scr[0, 1, at] = jnp.where(low, zero, swap).astype(jnp.bfloat16)
            scr[1, 0, at] = jnp.where(low, swap, zero).astype(jnp.bfloat16)
            scr[1, 1, at] = jnp.where(low, zero, both).astype(jnp.bfloat16)

    spread(0, own_ref)
    spread(1, left_ref)
    spread(2, right_ref)
    first_half = step < pl.num_programs(0) // 2

    @pl.when(first_half)
    def _():
        spread(3, opp_lo_ref)

    @pl.when(jnp.logical_not(first_half))
    def _():
        spread(3, opp_hi_ref)

    def one_pair(p, carry):
        cols = pl.ds(pl.multiple_of(p * pair, pair), pair)
        q_pair = q_ref[0, :, cols]
        group = p // (n_pairs // 2)
        out = None
        for side in range(2):
            s = lax.dot_general(q_pair, k_scr[group, side], (((1,), (1,)), ((), ())),
                                preferred_element_type=jnp.float32)
            s = jnp.minimum(s, bound_ref[...]) * score_c
            e = jnp.exp2(s - jnp.max(s, axis=-1, keepdims=True))
            probs = (e * (1.0 / jnp.sum(e, axis=-1, keepdims=True))).astype(jnp.bfloat16)
            part = jnp.dot(probs, v_scr[group, side], preferred_element_type=jnp.float32)
            out = part if out is None else out + part
        o_scr[:, cols] = out.astype(jnp.bfloat16)
        return carry

    lax.fori_loop(0, n_pairs, one_pair, 0, unroll=2)

    @pl.when(step == 0)
    def _():
        out_ref[...] = resid_ref[...].astype(jnp.float32)

    tok_n, width = wo_ref.shape[1], wo_ref.shape[3]
    for t in range(tok_n):
        at = slice(t * width, (t + 1) * width)
        out_ref[:, at] += jnp.dot(o_scr[...], wo_ref[0, t], preferred_element_type=jnp.float32)

    @pl.when(step == pl.num_programs(0) - 1)
    def _():
        hid_ref[...] = norm_rows(out_ref[...], gain_ref[...])


def attn_call(q, kvs, bound, wo_all, resid, gain, head_dim):
    shares, rows, q_w = q.shape
    kv2 = kvs[0].shape[2]
    embed = resid.shape[1]
    pair = kv2 // 2
    keys = bound.shape[1]
    heads = shares * q_w // head_dim
    part = shares // 2
    whole = pl.BlockSpec((1, rows, kv2), lambda m: (m, 0, 0))
    return pl.pallas_call(
        functools.partial(attn_kernel, LOG2_E * head_dim ** -0.5),
        name="attn",
        grid=(shares,),
        in_specs=[
            pl.BlockSpec((1, rows, q_w), lambda m: (m, 0, 0)),
            whole, whole, whole,
            pl.BlockSpec((1, rows, kv2), lambda m: (jnp.minimum(m, part - 1), 0, 0)),
            pl.BlockSpec((1, rows, kv2), lambda m: (jnp.maximum(m - part, 0), 0, 0)),
            pl.BlockSpec((rows, keys), lambda m: (0, 0)),
            pl.BlockSpec((1,) + wo_all.shape[1:], lambda m: (m, 0, 0, 0)),
            pl.BlockSpec((rows, embed), lambda m: (0, 0)),
            pl.BlockSpec((1, embed), lambda m: (0, 0)),
        ],
        out_specs=[
            pl.BlockSpec((rows, embed), lambda m: (0, 0)),
            pl.BlockSpec((rows, embed), lambda m: (0, 0)),
        ],
        out_shape=[
            jax.ShapeDtypeStruct((rows, embed), jnp.float32),
            jax.ShapeDtypeStruct((rows, embed), jnp.bfloat16),
        ],
        scratch_shapes=[
            pltpu.VMEM((2, 2, keys, pair), jnp.bfloat16),
            pltpu.VMEM((2, 2, keys, pair), jnp.bfloat16),
            pltpu.VMEM((rows, q_w), jnp.bfloat16),
        ],
        compiler_params=pltpu.CompilerParams(dimension_semantics=("arbitrary",), vmem_limit_bytes=40 * 1024 * 1024),
        cost_estimate=pl.CostEstimate(
            flops=2 * rows * q_w * embed * shares + 16 * heads * rows * keys * head_dim,
            bytes_accessed=2 * q_w * embed * shares, transcendentals=heads * rows * keys),
    )(q, *kvs, bound, wo_all, resid, gain)


def mlp_kernel(n_in, n_out, n_act, *refs):
    ins = refs[:n_in]
    wg_ref, wu_ref, wd_ref = refs[n_in:n_in + 3]
    outs = refs[n_in + 3:n_in + 3 + n_out]
    x_scr, act_scr = refs[-2:]
    step = pl.program_id(0)

    @pl.when(step == 0)
    def _():
        at = 0
        for ref in ins:
            x_scr[at:at + ref.shape[0]] = ref[...]
            at += ref.shape[0]

    @pl.when(step < n_act)
    def _():
        gate = jnp.dot(x_scr[...], wg_ref[...], preferred_element_type=jnp.float32)
        up = jnp.dot(x_scr[...], wu_ref[...], preferred_element_type=jnp.float32)
        act_scr[step] = (jax.nn.silu(gate) * up).astype(jnp.bfloat16)

    @pl.when(step >= n_act)
    def _():
        blk = act_scr.shape[2]
        part = None
        for i in range(n_act):
            term = jnp.dot(act_scr[i], wd_ref[i * blk:(i + 1) * blk], preferred_element_type=jnp.float32)
            part = term if part is None else part + term
        at = 0
        for ref in outs:
            ref[...] = part[at:at + ref.shape[0]]
            at += ref.shape[0]


def mlp_call(pieces, out_rows, w_g, w_u, w_d, blk=512, blk2=512):
    embed, ffn = w_g.shape
    total = sum(p.shape[0] for p in pieces)
    n_act = ffn // blk
    return pl.pallas_call(
        functools.partial(mlp_kernel, len(pieces), len(out_rows), n_act),
        name="mlp",
        grid=(n_act + embed // blk2,),
        in_specs=[pl.BlockSpec(p.shape, lambda f: (0, 0)) for p in pieces]
        + [
            pl.BlockSpec((embed, blk), lambda f: (0, jnp.minimum(f, n_act - 1))),
            pl.BlockSpec((embed, blk), lambda f: (0, jnp.minimum(f, n_act - 1))),
            pl.BlockSpec((ffn, blk2), lambda f: (0, jnp.maximum(f - n_act, 0))),
        ],
        out_specs=[pl.BlockSpec((r, blk2), lambda f: (0, jnp.maximum(f - n_act, 0))) for r in out_rows],
        out_shape=[jax.ShapeDtypeStruct((r, embed), jnp.float32) for r in out_rows],
        scratch_shapes=[pltpu.VMEM((total, embed), jnp.bfloat16), pltpu.VMEM((n_act, total, blk), jnp.bfloat16)],
        compiler_params=pltpu.CompilerParams(dimension_semantics=("arbitrary",), vmem_limit_bytes=48 * 1024 * 1024),
        cost_estimate=pl.CostEstimate(
            flops=6 * total * embed * ffn, bytes_accessed=6 * embed * ffn, transcendentals=total * ffn),
    )(*pieces, w_g, w_u, w_d)


def gather_kernel(mp_n, x_n, n_pieces, *refs):
    pieces, outs = refs[:n_pieces], refs[n_pieces:2 * n_pieces]
    local_sems, send_sems, x_full, x_half, y_full, y_half, side_sems = refs[2 * n_pieces:]
    j, t = lax.axis_index('mp'), lax.axis_index('tok')
    x, core = t // 2, t % 2
    x_near = {1: {'tok': lax.rem(x + 1, x_n) * 2 + core}, -1: {'tok': lax.rem(x + x_n - 1, x_n) * 2 + core}}
    y_near = {1: {'mp': lax.rem(j + 1, mp_n)}, -1: {'mp': lax.rem(j + mp_n - 1, mp_n)}}
    other = {'tok': x * 2 + 1 - core}

    barrier = pltpu.get_barrier_semaphore()
    partners = [x_near[1], x_near[-1], y_near[1], y_near[-1], other]
    for who in partners:
        pl.semaphore_signal(barrier, inc=1, device_id=who, device_id_type=pl.DeviceIdType.MESH)
    pl.semaphore_wait(barrier, len(partners))

    order = (0, -1, 1, 2)
    place = {d: i for i, d in enumerate(order)}
    near = tuple(enumerate((-1, 1)))
    sent = []

    def unit(n, dx, dj, c=None):
        at_t = lax.rem(x + dx + x_n, x_n) * 2 + (core if c is None else c)
        return outs[n].at[lax.rem(j + dj + mp_n, mp_n), at_t]

    def part(n, i, ref):
        half = pieces[n].shape[0] // 2
        return ref.at[i * half:(i + 1) * half]

    def send(src, dst, sem, who):
        copy = pltpu.make_async_remote_copy(
            src_ref=src, dst_ref=dst, send_sem=send_sems.at[len(sent)], recv_sem=sem,
            device_id=who, device_id_type=pl.DeviceIdType.MESH)
        copy.start()
        sent.append(copy)

    def arrived(dst, sem, who):
        pltpu.make_async_remote_copy(
            src_ref=dst, dst_ref=dst, send_sem=send_sems.at[0], recv_sem=sem,
            device_id=who, device_id_type=pl.DeviceIdType.MESH).wait_recv()

    def side_sem(n, dx, dj):
        return side_sems.at[n * 16 + place[dx] * 4 + place[dj]]

    def to_side(n, dx, dj, src):
        send(src, unit(n, dx, dj), side_sem(n, dx, dj), other)

    def to_rows(n, dx, src):
        send(src, unit(n, dx, 0), y_full.at[n * 8 + place[dx] * 2], y_near[1])
        send(src, unit(n, dx, 0), y_full.at[n * 8 + place[dx] * 2 + 1], y_near[-1])

    every = range(n_pieces)
    kept = []
    for n in every:
        own = pieces[n]
        keep = pltpu.make_async_copy(own, unit(n, 0, 0), local_sems.at[n])
        keep.start()
        kept.append(keep)
        for i, d in near:
            send(own, unit(n, 0, 0), x_full.at[n * 2 + i], x_near[-d])
        to_rows(n, 0, own)
        to_side(n, 0, 0, own)
    for n in every:
        for i, d in near:
            got = unit(n, d, 0)
            arrived(got, x_full.at[n * 2 + i], x_near[d])
            send(part(n, i, got), part(n, i, got), x_half.at[n * 2 + i], x_near[-d])
            to_rows(n, d, got)
            to_side(n, d, 0, got)
    for n in every:
        got = unit(n, 2, 0)
        for i, d in near:
            arrived(part(n, i, got), x_half.at[n * 2 + i], x_near[d])
        to_rows(n, 2, got)
        to_side(n, 2, 0, got)
    for n in every:
        for dx in order:
            for i, d in near:
                got = unit(n, dx, d)
                at = n * 8 + place[dx] * 2 + i
                arrived(got, y_full.at[at], y_near[d])
                send(part(n, i, got), part(n, i, got), y_half.at[at], y_near[-d])
                to_side(n, dx, d, got)
    for n in every:
        for dx in order:
            got = unit(n, dx, 2)
            for i, d in near:
                arrived(part(n, i, got), y_half.at[n * 8 + place[dx] * 2 + i], y_near[d])
            to_side(n, dx, 2, got)
    for n in every:
        for dx in order:
            for dj in order:
                arrived(unit(n, dx, dj, 1 - core), side_sem(n, dx, dj), other)
    for copy in sent:
        copy.wait_send()
    for keep in kept:
        keep.wait()


def gather_call(pieces, mp_n, tok_n):
    n = len(pieces)
    n_sends = 5 + 2 * 4 + 3 + 8 * 2 + 4
    dma = pltpu.SemaphoreType.DMA
    return pl.pallas_call(
        functools.partial(gather_kernel, mp_n, tok_n // 2, n),
        name="gather_weights",
        in_specs=[pl.BlockSpec(memory_space=pltpu.VMEM)] * n,
        out_specs=[pl.BlockSpec(memory_space=pl.ANY)] * n,
        out_shape=[jax.ShapeDtypeStruct((mp_n, tok_n) + p.shape, p.dtype) for p in pieces],
        scratch_shapes=[dma((n,)), dma((n * n_sends,)), dma((2 * n,)), dma((2 * n,)), dma((8 * n,)), dma((8 * n,)), dma((16 * n,))],
        compiler_params=pltpu.CompilerParams(collective_id=1, has_side_effects=True),
        cost_estimate=pl.CostEstimate(
            flops=10 ** 11, bytes_accessed=sum(p.size for p in pieces) * 2 * mp_n * tok_n, transcendentals=0),
    )(*pieces)


def solution(mesh):
    act_spec = P(None, ('rep', 'tok', 'mp'), None)
    seg_spec = P(None, ('rep', 'tok', 'mp'))
    gain_spec = P(None, None)
    head_in = P(None, 'tok', 'mp', None)
    head_out = P(None, 'mp', None, 'tok')
    ffn_in = P(None, 'tok', 'mp')
    ffn_out = P(None, 'mp', 'tok')
    mp_n, tok_n = mesh.shape['mp'], mesh.shape['tok']
    fwd = [(i, (i + 1) % mp_n) for i in range(mp_n)]
    bwd = [(i, (i - 1) % mp_n) for i in range(mp_n)]

    def to_right(value):
        return lax.ppermute(value, 'mp', fwd)

    def to_left(value):
        return lax.ppermute(value, 'mp', bwd)

    def spread_ring(value):
        half = value.shape[0] // 2
        from_left, from_right = to_right(value), to_left(value)
        return [value, from_left, from_right,
                to_right(from_left[:half]), to_left(from_right[half:])]

    def body(x_in, seg_ids, g_attn, w_q, w_k, w_v, w_o, g_mlp, w_gate, w_up, w_down):
        micro_n, rows, _ = x_in.shape
        layers = w_q.shape[0]
        head_dim = w_q.shape[3]
        e_part = w_q.shape[1]

        seg_parts = [seg_ids, to_right(seg_ids), to_left(seg_ids)]
        seg_parts.append(to_right(seg_parts[1]))
        me = lax.axis_index('mp')
        seg_ring = jnp.concatenate(seg_parts, axis=1)
        ring_at = [lax.rem(me + c + mp_n, mp_n) * rows for c in (0, -1, 1, 2)]
        key_at = jnp.concatenate([at + jnp.arange(rows, dtype=jnp.int32) for at in ring_at])
        own_at = key_at[:rows]
        streams = []
        for b in range(micro_n):
            same = seg_ring[b][None, :] == seg_ids[b][:, None]
            first = jnp.min(jnp.where(same, key_at[None, :], rows * mp_n), axis=1)
            cos_w, sin_w = rope_tables(own_at - first, head_dim)
            ok = same & (key_at[None, :] <= own_at[:, None])
            streams.append(dict(name='ab'[b], cos=cos_w, sin=sin_w, bound=jnp.where(ok, jnp.inf, -jnp.inf),
                                resid=x_in[b].astype(jnp.float32)))

        def gathered(value, axis_name, **how):
            return lax.all_gather(value, axis_name, **how)

        weights = []
        for l in range(layers):
            w_qkv = jnp.concatenate([w[l].reshape(e_part, -1) for w in (w_q, w_k, w_v)], axis=1)
            w_o_l = w_o[l].reshape(-1, w_o.shape[3])
            if l == 0:
                w_qkv, w_o_l, *_ = lax.optimization_barrier(
                    (w_qkv, w_o_l, *[st[k] for st in streams for k in ('cos', 'sin')]))
                w_qkv_all, w_o_all = gather_call([w_qkv, w_o_l], mp_n, tok_n)
                w_qkv_all = w_qkv_all.reshape(mp_n, tok_n * e_part, -1)
            else:
                w_qkv_all = gathered(gathered(w_qkv, 'mp', axis=0), 'tok', axis=1, tiled=True)
                w_o_all = gathered(gathered(w_o_l, 'mp', axis=0), 'tok', axis=1)
            weights.append((
                w_qkv_all, w_o_all,
                gathered(w_gate[l], 'tok', axis=0, tiled=True),
                gathered(w_up[l], 'tok', axis=0, tiled=True),
                gathered(w_down[l], 'tok', axis=1, tiled=True),
            ))

        half = rows // 2
        last = [None]

        def in_turn(value, *more):
            held = [v for v in (last[0],) + more if v is not None]
            return lax.optimization_barrier((value, *held))[0] if held else value

        def qkv_step(st, l):
            resid = in_turn(st['resid'])
            q, kv = qkv_call(resid, g_attn[l:l + 1], st['cos'], st['sin'], weights[l][0])
            st['q'], st['kvs'] = q, spread_ring(kv)
            last[0] = kv

        def attn_step(st, l, *more):
            q = in_turn(st['q'], *more)
            st['resid'], hid = attn_call(q, st['kvs'], st['bound'], weights[l][1], st['resid'],
                                         g_mlp[l:l + 1], head_dim)
            st['hid'] = last[0] = hid

        def share_step(st, *more):
            hid = lax.optimization_barrier((st['hid'], *more))[0] if more else st['hid']
            st['hids'] = spread_ring(hid)

        def opp_step(st, l):
            lo, hi = st['hids'][3:]
            lo = in_turn(lo)
            p_lo, p_hi = mlp_call([lo, hi], [half, half], *weights[l][2:])
            st['opp_in'] = to_right(p_lo), to_left(p_hi)
            last[0] = p_lo

        def near_step(st, l):
            own, left, right = st['hids'][:3]
            left = in_turn(left)
            p_own, left_lo, left_hi, right_lo, right_hi = mlp_call([own, left, right], [rows] + [half] * 4, *weights[l][2:])
            last[0] = p_own
            lo_in, hi_in = st['opp_in']
            hi_sum = to_right(right_hi)
            lo_sum = to_left(left_lo)
            lo_sum = lo_sum + to_right(right_lo + lo_in)
            hi_sum = hi_sum + to_left(left_hi + hi_in)
            st['resid'] = st['resid'] + p_own + jnp.concatenate([lo_sum, hi_sum], axis=0)

        a, b = streams
        for l in range(layers):
            qkv_step(a, l)
            if l == 0:
                qkv_step(b, l)
                attn_step(a, l)
                share_step(a)
                attn_step(b, l)
                share_step(b, *a['hids'][1:3])
                opp_step(a, l)
                near_step(a, l)
            else:
                attn_step(a, l)
                share_step(a)
                qkv_step(b, l)
                opp_step(a, l)
                attn_step(b, l)
                share_step(b)
                near_step(a, l)
            opp_step(b, l)
            near_step(b, l)
        return jnp.stack([st['resid'] for st in streams])


    return jax.shard_map(
        body,
        mesh=mesh,
        in_specs=(act_spec, seg_spec, gain_spec, head_in, head_in, head_in, head_out, gain_spec, ffn_in, ffn_in, ffn_out),
        out_specs=act_spec,
        check_vma=False,
    )
```
